256 devices in a mesh: dp: 2 (over x_lo), expert: 128 (over y, z, x_hi, core).
Axes of the slice: x: 4 (x_hi: 2, x_lo: 2; x = x_hi * 2 + x_lo), y: 4, z: 8, core: 2. Of those that a mesh axis runs over, the one named last changes fastest.
Arguments:
- tokens: bfloat16 [256, 256, 1280], P(('dp', 'expert')), may hold values from -12 to 12
- router: bfloat16 [1280, 128], replicated, may hold values from -3 to 3
- w_in: bfloat16 [128, 1280, 5120], P('expert', None, 'dp'), may hold values from -0.15625 to 0.15625
- b_in: bfloat16 [128, 5120], P('expert'), may hold values from -3 to 3
- w_out: bfloat16 [128, 5120, 1280], P('expert', 'dp'), may hold values from -0.078125 to 0.078125
- b_out: bfloat16 [128, 1280], P('expert'), may hold values from -3 to 3
Outputs:
- mixed: bfloat16 [256, 256, 1280], P(('dp', 'expert'))
The draws below stay inside these ranges and needn't reach their ends.
All inputs are finite; a program needn't handle non-finite values.
Results may differ from the reference program's by a relative error of at most 0.014.
Values may be sent and summed in bfloat16 or wider, within the bound.
A program may use at most 64 MiB of HBM per device.

```python
import math
import jax
import jax.numpy as jnp
from jax import lax

D = 1280
HID = 5120
M = 256
EXPERTS = 128
IMAGES = 256


def image_tokens(base, index):
    image_key = jax.random.fold_in(base, index)
    values = jnp.clip(jax.random.normal(jax.random.fold_in(image_key, 1), (M, D), jnp.float32), -6.0, 6.0)
    return values


def draw_tokens(key, part):
    base = jax.random.fold_in(key, 11)
    stacked = jax.vmap(lambda index: image_tokens(base, index))(jnp.arange(IMAGES))
    return stacked.astype(jnp.bfloat16)


def draw_router(key, part):
    values = jax.random.normal(jax.random.fold_in(key, 12), (D, EXPERTS), jnp.float32) * (2.5 / math.sqrt(D))
    values = jnp.clip(values, -0.5, 0.5)
    return values.astype(jnp.bfloat16)


def shard_levels(key, dims, cuts, low, top_value):
    def one(dim, parts):
        draws = jax.random.uniform(jax.random.fold_in(jax.random.fold_in(key, 6), dim), (parts,), jnp.float32, low / len(cuts), top_value / len(cuts))
        return jnp.repeat(jnp.exp(draws), dims[dim] // parts).reshape((-1,) + (1,) * (len(dims) - dim - 1))

    gain = one(*cuts[0])
    for cut in cuts[1:]:
        gain = gain * one(*cut)
    return gain


def bell_draw(stream_key, dims, deviation, reach, cuts=(), dtype=jnp.bfloat16):
    factor_of = shard_levels(stream_key, dims, cuts, -0.22, 0.18) if cuts else 1.0
    array = jax.random.normal(stream_key, dims, jnp.float32) * deviation * factor_of
    return jnp.minimum(jnp.maximum(array, -reach), reach).astype(dtype)


def setup_inputs(seed: int = 0) -> dict:
    splits = jax.random.split(jax.random.key(seed), 7)
    tokens = draw_tokens(jax.random.fold_in(splits[6], 71), 0)
    router = draw_router(jax.random.fold_in(splits[6], 71), 0)
    w_in = bell_draw(splits[2], (EXPERTS, D, HID), D ** -0.5, 0.15625, ((0, 128), (2, 2)))
    b_in = bell_draw(splits[3], (EXPERTS, HID), 0.5, 3.0, ((0, 128),))
    w_out = bell_draw(splits[4], (EXPERTS, HID, D), HID ** -0.5, 0.078125, ((0, 128), (1, 2)))
    b_out = bell_draw(splits[5], (EXPERTS, D), 0.5, 3.0, ((0, 128),))
    return {"tokens": tokens, "router": router, "w_in": w_in, "b_in": b_in, "w_out": w_out, "b_out": b_out}


def run_expert(packed):
    slot_rows, weight_in, bias_in, weight_out, bias_out = packed
    hidden = jax.nn.gelu(jnp.dot(slot_rows, weight_in, preferred_element_type=jnp.float32) + bias_in.astype(jnp.float32), approximate=False).astype(jnp.bfloat16)
    return (jnp.dot(hidden, weight_out, preferred_element_type=jnp.float32) + bias_out.astype(jnp.float32)).astype(jnp.bfloat16)


def reference(tokens, router, w_in, b_in, w_out, b_out):
    logits = jnp.einsum("bmd,de->bme", tokens.astype(jnp.float32), router.astype(jnp.float32))
    dispatch = jax.nn.softmax(logits, axis=1).astype(jnp.bfloat16)
    combine = jax.nn.softmax(logits, axis=2).astype(jnp.bfloat16)
    slots = jnp.einsum("bme,bmd->ebd", dispatch.astype(jnp.float32), tokens.astype(jnp.float32)).astype(jnp.bfloat16)
    expert_out = lax.map(run_expert, (slots, w_in, b_in, w_out, b_out))
    mixed = jnp.einsum("bme,ebd->bmd", combine.astype(jnp.float32), expert_out.astype(jnp.float32))
    return mixed.astype(jnp.bfloat16)
```

```python
import functools
import jax
import jax.numpy as jnp
from jax import lax
from jax.experimental import pallas as pl
from jax.experimental.pallas import tpu as pltpu
from jax.sharding import Mesh
from jax.sharding import PartitionSpec as P

AXES = ("dp", "y", "z", "xh", "core")
EXPERT = ("y", "z", "xh", "core")
F32 = jnp.float32
BF16 = jnp.bfloat16
LOGICAL = pl.DeviceIdType.LOGICAL
NY, NZ = 4, 8
EXPERTS = 128
HALF = 640
BATCH = 64
GROUP = 16
SLOTS = [(dy, dz, dx, dc) for dy in range(NY) for dz in range(NZ) for dx in range(2) for dc in range(2)]


def hops(place):
    dy, dz, dx, _ = place
    return min(dy, NY - dy) + min(dz, NZ - dz) + dx


def one_hot(shape, col_of_row):
    rows = lax.broadcasted_iota(jnp.int32, shape, 0)
    cols = lax.broadcasted_iota(jnp.int32, shape, 1)
    return jnp.where(cols == col_of_row(rows), 1.0, 0.0).astype(BF16)


def spread(shape, h):
    rows = lax.broadcasted_iota(jnp.int32, shape, 0)
    cols = lax.broadcasted_iota(jnp.int32, shape, 1)
    return jnp.where(cols == 2 * rows + h, 1.0, 0.0).astype(BF16)


def spread_t(shape, h):
    rows = lax.broadcasted_iota(jnp.int32, shape, 0)
    cols = lax.broadcasted_iota(jnp.int32, shape, 1)
    return jnp.where(rows == 2 * cols + h, 1.0, 0.0).astype(BF16)


def dot(a, b):
    return jnp.dot(a, b, preferred_element_type=F32)


def dot_nt(a, b):
    return lax.dot_general(a, b, (((1,), (1,)), ((), ())), preferred_element_type=F32)


def gelu(v):
    return v * (1.0 + lax.erf(v * 0.7071067811865476)) * 0.5


def kernel(
    tokens_h, router_h, w_in_h, b_in_h, w_out_h, b_out_h, out_ref,
    tok, router, w_in, w_out, b_in, b_out, src, got, got2, x, hidden, part, psend, precv, rsrc, ret, comb2, self2, unit,
    load_sem, w_sem, send_sem, recv_sem, fsend_sem, frecv_sem, psend_sem, precv_sem, rsend_sem, rrecv_sem,
):
    dp, y, z, xh, c = (lax.axis_index(a) for a in AXES)
    ys = [lax.rem(y + k, NY) * 32 for k in range(NY)]
    zs = [lax.rem(z + k, NZ) * 4 for k in range(NZ)]
    xs = [xh * 2, (1 - xh) * 2]
    cs = [c, 1 - c]
    ds = [dp * EXPERTS, (1 - dp) * EXPERTS]
    me = ys[0] + zs[0] + xs[0] + cs[0]
    partner = me + ds[1]

    def expert_at(place, sign=1):
        dy, dz, dx, dc = place
        return ys[(sign * dy) % NY] + zs[(sign * dz) % NZ] + xs[dx] + cs[dc]

    def device_at(place, sign=1):
        return expert_at(place, sign) + ds[place[2]]

    half = w_in.shape[1]
    loads = [
        pltpu.make_async_copy(tokens_h.at[0], tok, load_sem.at[0]),
        pltpu.make_async_copy(router_h, router, load_sem.at[1]),
        pltpu.make_async_copy(b_in_h.at[:, pl.ds(pl.multiple_of(dp * half, half), half)], b_in, load_sem.at[2]),
        pltpu.make_async_copy(b_out_h, b_out, load_sem.at[3]),
    ]
    weights = [
        pltpu.make_async_copy(w_in_h.at[0], w_in, w_sem.at[0]),
        pltpu.make_async_copy(w_out_h.at[0], w_out, w_sem.at[1]),
    ]
    for copy in loads[:2]:
        copy.start()
    ret[...] = jnp.zeros_like(ret)

    barrier = pltpu.get_barrier_semaphore()
    for place in sorted(SLOTS[1:], key=hops, reverse=True):
        pl.semaphore_signal(barrier, inc=1, device_id=device_at(place), device_id_type=LOGICAL)
    pl.semaphore_signal(barrier, inc=1, device_id=partner, device_id_type=LOGICAL)
    for copy in loads[2:] + weights:
        copy.start()

    for copy in loads[:2]:
        copy.wait()
    logits = dot(tok[...], router[...])
    up = jnp.exp(logits - jnp.max(logits, axis=0, keepdims=True))
    dispatch = (up / jnp.sum(up, axis=0, keepdims=True)).astype(BF16)
    across = jnp.exp(logits - jnp.max(logits, axis=1, keepdims=True))
    combine = (across / jnp.sum(across, axis=1, keepdims=True)).astype(BF16)
    rows = None
    for h in range(2):
        lhs = dot_nt(spread_t((2 * EXPERTS, EXPERTS), h), dispatch).astype(BF16)
        term = dot(lhs, tok[:, h * HALF : (h + 1) * HALF])
        rows = term if rows is None else rows + term
        comb2[h] = dot(combine, spread((EXPERTS, 2 * EXPERTS), h)).astype(BF16)
        pick = lax.broadcasted_iota(jnp.int32, (EXPERTS, 2 * BATCH), 0) == me
        into = lax.broadcasted_iota(jnp.int32, (EXPERTS, 2 * BATCH), 1) == h
        self2[h] = dot(combine, jnp.where(pick & into, 1.0, 0.0).astype(BF16)).astype(BF16)
    src[...] = rows.astype(BF16)
    mine = dot(one_hot((8, 2 * EXPERTS), lambda r: 2 * me + r), src[...]).astype(BF16)
    got[0:2, :] = mine[0:2, :]

    pl.semaphore_wait(barrier, len(SLOTS))

    for k, place in enumerate(SLOTS):
        if k == 0:
            continue
        pltpu.make_async_remote_copy(
            src.at[pl.ds(pl.multiple_of(2 * expert_at(place), 2), 2)],
            got.at[pl.ds(2 * k, 2)],
            send_sem, recv_sem.at[k // GROUP],
            device_id=device_at(place), device_id_type=LOGICAL,
        ).start()

    def forward(g):
        held = unit.at[pl.ds(0, GROUP - 1 if g == 0 else GROUP)]
        pltpu.make_async_copy(held, held, recv_sem.at[g]).wait()
        block = pl.ds(2 * GROUP * g, 2 * GROUP)
        pltpu.make_async_remote_copy(
            got.at[block], got2.at[block], fsend_sem, frecv_sem.at[2 * GROUP * g // (2 * BATCH)],
            device_id=partner, device_id_type=LOGICAL,
        ).start()

    groups = EXPERTS // GROUP
    width = w_in.shape[0]

    def first_half(b):
        block = pl.ds(2 * BATCH * b, 2 * BATCH)
        pltpu.make_async_copy(got2.at[block], got2.at[block], frecv_sem.at[b]).wait()
        for h in range(2):
            order = spread((BATCH, 2 * BATCH), h)
            x[0:BATCH, h * HALF : (h + 1) * HALF] = dot(order, got[block, :]).astype(BF16)
            x[BATCH : 2 * BATCH, h * HALF : (h + 1) * HALF] = dot(order, got2[block, :]).astype(BF16)
        if b == 0:
            loads[2].wait()
            weights[0].wait()
        step = 512
        for j in range(half // step):
            cols = slice(j * step, (j + 1) * step)
            acc = dot(x[...], w_in[:, cols]) + b_in[:, cols].astype(F32)
            hidden[:, cols] = gelu(acc).astype(BF16)

    def second_half(b):
        if b == 0:
            weights[1].wait()
        step = 256
        for j in range(width // step):
            cols = slice(j * step, (j + 1) * step)
            acc = dot(hidden[...], w_out[:, cols])
            part[b, :, cols] = acc[0:BATCH]
            psend[b, :, cols] = acc[BATCH : 2 * BATCH].astype(BF16)
        pltpu.make_async_remote_copy(
            psend.at[b], precv.at[b], psend_sem, precv_sem.at[b], device_id=partner, device_id_type=LOGICAL
        ).start()

    def send_back(b):
        pltpu.make_async_copy(precv.at[b], precv.at[b], precv_sem.at[b]).wait()
        if b == 0:
            loads[3].wait()
        result = (part[b] + precv[b].astype(F32) + b_out[...].astype(F32)).astype(BF16)
        rows = None
        for h in range(2):
            term = dot(spread_t((2 * BATCH, BATCH), h), result[:, h * HALF : (h + 1) * HALF])
            rows = term if rows is None else rows + term
        rsrc[b] = rows.astype(BF16)
        for i in range(BATCH):
            k = BATCH * b + i
            if k == 0:
                continue
            pltpu.make_async_remote_copy(
                rsrc.at[b, pl.ds(2 * i, 2)],
                ret.at[pl.ds(pl.multiple_of(2 * me, 2), 2)],
                rsend_sem, rrecv_sem,
                device_id=device_at(SLOTS[k], -1), device_id_type=LOGICAL,
            ).start()

    for g in range(groups // 2):
        forward(g)
    first_half(0)
    for g in range(groups // 2, groups):
        forward(g)
    second_half(0)
    first_half(1)
    send_back(0)
    second_half(1)
    send_back(1)

    others = unit.at[pl.ds(0, EXPERTS - 1)]
    pltpu.make_async_copy(others, others, rrecv_sem).wait()
    for h in range(2):
        mixed = dot(comb2[h], ret[...]) + dot(self2[h], rsrc[0])
        out_ref[:, h * HALF : (h + 1) * HALF] = mixed.astype(BF16)

    pltpu.make_async_copy(others, others, send_sem).wait()
    pltpu.make_async_copy(others, others, rsend_sem).wait()
    pltpu.make_async_copy(got, got, fsend_sem).wait()
    pltpu.make_async_copy(psend, psend, psend_sem).wait()


def layer(tokens, router, w_in, b_in, w_out, b_out):
    _, m, d = tokens.shape
    half = w_in.shape[2]
    anywhere = pl.BlockSpec(memory_space=pl.ANY)
    dma = pltpu.SemaphoreType.DMA
    out = pl.pallas_call(
        kernel,
        name="soft_moe",
        out_shape=jax.ShapeDtypeStruct((m, d), BF16),
        in_specs=[anywhere] * 6,
        out_specs=pl.BlockSpec(memory_space=pltpu.VMEM),
        scratch_shapes=[
            pltpu.VMEM((m, d), BF16),
            pltpu.VMEM((d, EXPERTS), BF16),
            pltpu.VMEM((d, half), BF16),
            pltpu.VMEM((half, d), BF16),
            pltpu.VMEM((1, half), BF16),
            pltpu.VMEM((1, d), BF16),
            pltpu.VMEM((2 * EXPERTS, HALF), BF16),
            pltpu.VMEM((2 * EXPERTS, HALF), BF16),
            pltpu.VMEM((2 * EXPERTS, HALF), BF16),
            pltpu.VMEM((2 * BATCH, d), BF16),
            pltpu.VMEM((2 * BATCH, half), BF16),
            pltpu.VMEM((2, BATCH, d), F32),
            pltpu.VMEM((2, BATCH, d), BF16),
            pltpu.VMEM((2, BATCH, d), BF16),
            pltpu.VMEM((2, 2 * BATCH, HALF), BF16),
            pltpu.VMEM((2 * EXPERTS, HALF), BF16),
            pltpu.VMEM((2, m, 2 * EXPERTS), BF16),
            pltpu.VMEM((2, m, 2 * BATCH), BF16),
            pltpu.VMEM((EXPERTS, 2, HALF), BF16),
            dma((4,)), dma((2,)),
            dma, dma((EXPERTS // GROUP,)),
            dma, dma((2,)),
            dma, dma((2,)),
            dma, dma,
        ],
        compiler_params=pltpu.CompilerParams(
            collective_id=1, has_side_effects=True, vmem_limit_bytes=48 * 1024 * 1024
        ),
    )(tokens, router, w_in, b_in, w_out, b_out)
    return out[None]


def solution(mesh):
    finer = Mesh(mesh.devices.reshape(mesh.shape["dp"], NY, NZ, 2, 2), AXES)
    return jax.shard_map(
        layer,
        mesh=finer,
        in_specs=(
            P(AXES, None, None),
            P(),
            P(EXPERT, None, "dp"),
            P(EXPERT, None),
            P(EXPERT, "dp", None),
            P(EXPERT, None),
        ),
        out_specs=P(AXES, None, None),
        check_vma=False,
    )
```

```python
import functools
import jax
import jax.numpy as jnp
from jax import lax
from jax.experimental import pallas as pl
from jax.experimental.pallas import tpu as pltpu
from jax.sharding import Mesh
from jax.sharding import PartitionSpec as P

AXES = ("dp", "y", "z", "xh", "core")
EXPERT = ("y", "z", "xh", "core")
F32 = jnp.float32
BF16 = jnp.bfloat16
LOGICAL = pl.DeviceIdType.LOGICAL
NY, NZ = 4, 8
EXPERTS = 128
HALF = 640


def hops(place):
    dy, dz, dx, _ = place
    return min(dy, NY - dy) + min(dz, NZ - dz) + dx


PLACES = sorted(
    ((dy, dz, dx, dc) for dy in range(NY) for dz in range(NZ) for dx in range(2) for dc in range(2)), key=hops
)
ORDER = "O1"
SLOTS = {
    "O1": PLACES,
    "O2": PLACES[::-1],
    "O3": PLACES[:32] + PLACES[96:] + PLACES[64:96] + PLACES[32:64],
    "O4": sorted(PLACES),
}[ORDER]
SELF = SLOTS.index((0, 0, 0, 0))
SIZES = (32, 32, 32, 32)
BATCHES = [(sum(SIZES[:b]), n) for b, n in enumerate(SIZES)]
SCHEDULE = "F0 F1 G0 H0 F2 G1 H1 R0 F3 G2 H2 R1 G3 H3 R2 R3"

def one_hot(shape, col_of_row):
    rows = lax.broadcasted_iota(jnp.int32, shape, 0)
    cols = lax.broadcasted_iota(jnp.int32, shape, 1)
    return jnp.where(cols == col_of_row(rows), 1.0, 0.0).astype(BF16)


def spread(shape, h):
    rows = lax.broadcasted_iota(jnp.int32, shape, 0)
    cols = lax.broadcasted_iota(jnp.int32, shape, 1)
    return jnp.where(cols == 2 * rows + h, 1.0, 0.0).astype(BF16)


def spread_t(shape, h):
    rows = lax.broadcasted_iota(jnp.int32, shape, 0)
    cols = lax.broadcasted_iota(jnp.int32, shape, 1)
    return jnp.where(rows == 2 * cols + h, 1.0, 0.0).astype(BF16)


def dot(a, b):
    return jnp.dot(a, b, preferred_element_type=F32)


def dot_nt(a, b):
    return lax.dot_general(a, b, (((1,), (1,)), ((), ())), preferred_element_type=F32)


def gelu(v):
    return v * (1.0 + lax.erf(v * 0.7071067811865476)) * 0.5


def kernel(
    tokens_h, router_h, w_in_h, b_in_h, w_out_h, b_out_h, out_ref,
    tok, router, w_in, w_out, b_in, b_out, src, got, got2, x, hidden, part, psend, precv, rsrc, ret, comb2, self2, unit,
    load_sem, w_sem, send_sem, recv_sem, fsend_sem, frecv_sem, psend_sem, precv_sem, rsend_sem, rrecv_sem,
):
    dp, y, z, xh, c = (lax.axis_index(a) for a in AXES)
    ys = [lax.rem(y + k, NY) * 32 for k in range(NY)]
    zs = [lax.rem(z + k, NZ) * 4 for k in range(NZ)]
    xs = [xh * 2, (1 - xh) * 2]
    cs = [c, 1 - c]
    ds = [dp * EXPERTS, (1 - dp) * EXPERTS]
    me = ys[0] + zs[0] + xs[0] + cs[0]
    partner = me + ds[1]

    def expert_at(place, sign=1):
        dy, dz, dx, dc = place
        return ys[(sign * dy) % NY] + zs[(sign * dz) % NZ] + xs[dx] + cs[dc]

    def device_at(place, sign=1):
        return expert_at(place, sign) + ds[place[2]]

    half = w_in.shape[1]
    loads = [
        pltpu.make_async_copy(tokens_h.at[0], tok, load_sem.at[0]),
        pltpu.make_async_copy(router_h, router, load_sem.at[1]),
        pltpu.make_async_copy(b_in_h.at[:, pl.ds(pl.multiple_of(dp * half, half), half)], b_in, load_sem.at[2]),
        pltpu.make_async_copy(b_out_h, b_out, load_sem.at[3]),
    ]
    weights = [
        pltpu.make_async_copy(w_in_h.at[0], w_in, w_sem.at[0]),
        pltpu.make_async_copy(w_out_h.at[0], w_out, w_sem.at[1]),
    ]
    for copy in loads[:2]:
        copy.start()
    ret[...] = jnp.zeros_like(ret)

    barrier = pltpu.get_barrier_semaphore()
    for place in sorted(SLOTS[1:], key=hops, reverse=True):
        pl.semaphore_signal(barrier, inc=1, device_id=device_at(place), device_id_type=LOGICAL)
    pl.semaphore_signal(barrier, inc=1, device_id=partner, device_id_type=LOGICAL)
    for copy in loads[2:] + weights:
        copy.start()

    self_block, self_row = 2 * SELF // EXPERTS, 2 * SELF % EXPERTS
    for copy in loads[:2]:
        copy.wait()
    logits = dot(tok[...], router[...])
    up = jnp.exp(logits - jnp.max(logits, axis=0, keepdims=True))
    dispatch = (up / jnp.sum(up, axis=0, keepdims=True)).astype(BF16)
    across = jnp.exp(logits - jnp.max(logits, axis=1, keepdims=True))
    combine = (across / jnp.sum(across, axis=1, keepdims=True)).astype(BF16)
    rows = None
    for h in range(2):
        lhs = dot_nt(spread_t((2 * EXPERTS, EXPERTS), h), dispatch).astype(BF16)
        term = dot(lhs, tok[:, h * HALF : (h + 1) * HALF])
        rows = term if rows is None else rows + term
        comb2[h] = dot(combine, spread((EXPERTS, 2 * EXPERTS), h)).astype(BF16)
        pick = lax.broadcasted_iota(jnp.int32, (EXPERTS, EXPERTS), 0) == me
        into = lax.broadcasted_iota(jnp.int32, (EXPERTS, EXPERTS), 1) == self_row + h
        self2[h] = dot(combine, jnp.where(pick & into, 1.0, 0.0).astype(BF16)).astype(BF16)
    src[...] = rows.astype(BF16)
    mine = dot(one_hot((8, 2 * EXPERTS), lambda r: 2 * me + r), src[...]).astype(BF16)
    got[2 * SELF : 2 * SELF + 2, :] = mine[0:2, :]

    pl.semaphore_wait(barrier, len(SLOTS))

    for b, (first, count) in enumerate(BATCHES):
        for k in range(first, first + count):
            if k != SELF:
                pltpu.make_async_remote_copy(
                    src.at[pl.ds(pl.multiple_of(2 * expert_at(SLOTS[k]), 2), 2)],
                    got.at[pl.ds(2 * k, 2)],
                    send_sem, recv_sem.at[b],
                    device_id=device_at(SLOTS[k]), device_id_type=LOGICAL,
                ).start()

    width = w_in.shape[0]

    def forward(b):
        first, count = BATCHES[b]
        held = unit.at[pl.ds(0, count - 1 if first <= SELF < first + count else count)]
        pltpu.make_async_copy(held, held, recv_sem.at[b]).wait()
        block = pl.ds(2 * first, 2 * count)
        pltpu.make_async_remote_copy(
            got.at[block], got2.at[block], fsend_sem, frecv_sem.at[b], device_id=partner, device_id_type=LOGICAL
        ).start()

    def first_half(b):
        first, count = BATCHES[b]
        block = pl.ds(2 * first, 2 * count)
        pltpu.make_async_copy(got2.at[block], got2.at[block], frecv_sem.at[b]).wait()
        for h in range(2):
            order = spread((count, 2 * count), h)
            x[0:count, h * HALF : (h + 1) * HALF] = dot(order, got[block, :]).astype(BF16)
            x[count : 2 * count, h * HALF : (h + 1) * HALF] = dot(order, got2[block, :]).astype(BF16)
        if b == 0:
            loads[2].wait()
            weights[0].wait()
        step = 512
        for j in range(half // step):
            cols = slice(j * step, (j + 1) * step)
            acc = dot(x[0 : 2 * count], w_in[:, cols]) + b_in[:, cols].astype(F32)
            hidden[0 : 2 * count, cols] = gelu(acc).astype(BF16)

    def second_half(b):
        first, count = BATCHES[b]
        block = pl.ds(first, count)
        if b == 0:
            weights[1].wait()
        step = 256
        for j in range(width // step):
            cols = slice(j * step, (j + 1) * step)
            acc = dot(hidden[0 : 2 * count], w_out[:, cols])
            part[block, cols] = acc[0:count]
            psend[block, cols] = acc[count : 2 * count].astype(BF16)
        pltpu.make_async_remote_copy(
            psend.at[block], precv.at[block], psend_sem, precv_sem.at[b], device_id=partner, device_id_type=LOGICAL
        ).start()

    def send_back(b):
        first, count = BATCHES[b]
        block = pl.ds(first, count)
        pltpu.make_async_copy(precv.at[block], precv.at[block], precv_sem.at[b]).wait()
        if b == 0:
            loads[3].wait()
        result = (part[block, :] + precv[block, :].astype(F32) + b_out[...].astype(F32)).astype(BF16)
        rows = None
        for h in range(2):
            term = dot(spread_t((2 * count, count), h), result[:, h * HALF : (h + 1) * HALF])
            rows = term if rows is None else rows + term
        rsrc[pl.ds(2 * first, 2 * count), :] = rows.astype(BF16)
        for k in range(first, first + count):
            if k != SELF:
                pltpu.make_async_remote_copy(
                    rsrc.at[pl.ds(2 * k, 2)],
                    ret.at[pl.ds(pl.multiple_of(2 * me, 2), 2)],
                    rsend_sem, rrecv_sem,
                    device_id=device_at(SLOTS[k], -1), device_id_type=LOGICAL,
                ).start()

    stages = {"F": forward, "G": first_half, "H": second_half, "R": send_back}
    for stage in SCHEDULE.split():
        stages[stage[0]](int(stage[1:]))

    others = unit.at[pl.ds(0, EXPERTS - 1)]
    pltpu.make_async_copy(others, others, rrecv_sem).wait()
    for h in range(2):
        own = rsrc[self_block * EXPERTS : (self_block + 1) * EXPERTS, :]
        mixed = dot(comb2[h], ret[...]) + dot(self2[h], own)
        out_ref[:, h * HALF : (h + 1) * HALF] = mixed.astype(BF16)

    pltpu.make_async_copy(others, others, send_sem).wait()
    pltpu.make_async_copy(others, others, rsend_sem).wait()
    pltpu.make_async_copy(got, got, fsend_sem).wait()
    pltpu.make_async_copy(psend, psend, psend_sem).wait()


def layer(tokens, router, w_in, b_in, w_out, b_out):
    _, m, d = tokens.shape
    half = w_in.shape[2]
    anywhere = pl.BlockSpec(memory_space=pltpu.HBM)
    dma = pltpu.SemaphoreType.DMA
    out = pl.pallas_call(
        kernel,
        name="soft_moe",
        out_shape=jax.ShapeDtypeStruct((m, d), BF16),
        in_specs=[anywhere] * 6,
        out_specs=pl.BlockSpec(memory_space=pltpu.VMEM),
        scratch_shapes=[
            pltpu.VMEM((m, d), BF16),
            pltpu.VMEM((d, EXPERTS), BF16),
            pltpu.VMEM((d, half), BF16),
            pltpu.VMEM((half, d), BF16),
            pltpu.VMEM((1, half), BF16),
            pltpu.VMEM((1, d), BF16),
            pltpu.VMEM((2 * EXPERTS, HALF), BF16),
            pltpu.VMEM((2 * EXPERTS, HALF), BF16),
            pltpu.VMEM((2 * EXPERTS, HALF), BF16),
            pltpu.VMEM((2 * max(SIZES), d), BF16),
            pltpu.VMEM((2 * max(SIZES), half), BF16),
            pltpu.VMEM((EXPERTS, d), F32),
            pltpu.VMEM((EXPERTS, d), BF16),
            pltpu.VMEM((EXPERTS, d), BF16),
            pltpu.VMEM((2 * EXPERTS, HALF), BF16),
            pltpu.VMEM((2 * EXPERTS, HALF), BF16),
            pltpu.VMEM((2, m, 2 * EXPERTS), BF16),
            pltpu.VMEM((2, m, EXPERTS), BF16),
            pltpu.VMEM((EXPERTS, 2, HALF), BF16),
            dma((4,)), dma((2,)),
            dma, dma((len(SIZES),)),
            dma, dma((len(SIZES),)),
            dma, dma((len(SIZES),)),
            dma, dma,
        ],
        compiler_params=pltpu.CompilerParams(
            collective_id=1, has_side_effects=True, vmem_limit_bytes=67043328
        ),
    )(tokens, router, w_in, b_in, w_out, b_out)
    return out[None]


def solution(mesh):
    finer = Mesh(mesh.devices.reshape(mesh.shape["dp"], NY, NZ, 2, 2), AXES)
    return jax.shard_map(
        layer,
        mesh=finer,
        in_specs=(
            P(AXES, None, None),
            P(),
            P(EXPERT, None, "dp"),
            P(EXPERT, None),
            P(EXPERT, "dp", None),
            P(EXPERT, None),
        ),
        out_specs=P(AXES, None, None),
        check_vma=False,
    )
```

```python
import functools
import jax
import jax.numpy as jnp
from jax import lax
from jax.experimental import pallas as pl
from jax.experimental.pallas import tpu as pltpu
from jax.sharding import Mesh
from jax.sharding import PartitionSpec as P

AXES = ("dp", "y", "z", "xh", "core")
EXPERT = ("y", "z", "xh", "core")
F32 = jnp.float32
BF16 = jnp.bfloat16
LOGICAL = pl.DeviceIdType.LOGICAL
NY, NZ = 4, 8
EXPERTS = 128
HALF = 640


def hops(place):
    dy, dz, dx, _ = place
    return min(dy, NY - dy) + min(dz, NZ - dz) + dx


PLACES = sorted(
    ((dy, dz, dx, dc) for dy in range(NY) for dz in range(NZ) for dx in range(2) for dc in range(2)), key=hops
)
ORDER = "O1"
SLOTS = {
    "O1": PLACES,
    "O2": PLACES[::-1],
    "O3": PLACES[:32] + PLACES[96:] + PLACES[64:96] + PLACES[32:64],
    "O4": sorted(PLACES),
    "O5": PLACES[:64] + PLACES[96:] + PLACES[64:96],
    "O6": PLACES[:32] + PLACES[64:] + PLACES[32:64],
}[ORDER]
SELF = SLOTS.index((0, 0, 0, 0))
SIZES = (32, 32, 32, 32)
BATCHES = [(sum(SIZES[:b]), n) for b, n in enumerate(SIZES)]
SCHEDULE = ("F0", "F1", "G0", "F2", "H0", "F3", "G1", "H1", "G2", "R0", "H2", "G3", "R1", "H3", "R2", "R3")

def one_hot(shape, col_of_row):
    rows = lax.broadcasted_iota(jnp.int32, shape, 0)
    cols = lax.broadcasted_iota(jnp.int32, shape, 1)
    return jnp.where(cols == col_of_row(rows), 1.0, 0.0).astype(BF16)


def spread(shape, h):
    rows = lax.broadcasted_iota(jnp.int32, shape, 0)
    cols = lax.broadcasted_iota(jnp.int32, shape, 1)
    return jnp.where(cols == 2 * rows + h, 1.0, 0.0).astype(BF16)


def spread_t(shape, h):
    rows = lax.broadcasted_iota(jnp.int32, shape, 0)
    cols = lax.broadcasted_iota(jnp.int32, shape, 1)
    return jnp.where(rows == 2 * cols + h, 1.0, 0.0).astype(BF16)


def dot(a, b):
    return jnp.dot(a, b, preferred_element_type=F32)


def dot_nt(a, b):
    return lax.dot_general(a, b, (((1,), (1,)), ((), ())), preferred_element_type=F32)


def gelu(v):
    return v * (1.0 + lax.erf(v * 0.7071067811865476)) * 0.5


def kernel(
    tokens_h, router_h, w_in_h, b_in_h, w_out_h, b_out_h, out_ref,
    tok, router, w_in, w_out, b_in, b_out, src, got, got2, x, hidden, part, psend, precv, rsrc, ret, comb2, self2, unit,
    load_sem, w_sem, send_sem, recv_sem, fsend_sem, frecv_sem, psend_sem, precv_sem, rsend_sem, rrecv_sem,
):
    dp, y, z, xh, c = (lax.axis_index(a) for a in AXES)
    ys = [lax.rem(y + k, NY) * 32 for k in range(NY)]
    zs = [lax.rem(z + k, NZ) * 4 for k in range(NZ)]
    xs = [xh * 2, (1 - xh) * 2]
    cs = [c, 1 - c]
    ds = [dp * EXPERTS, (1 - dp) * EXPERTS]
    me = ys[0] + zs[0] + xs[0] + cs[0]
    partner = me + ds[1]

    def expert_at(place, sign=1):
        dy, dz, dx, dc = place
        return ys[(sign * dy) % NY] + zs[(sign * dz) % NZ] + xs[dx] + cs[dc]

    def device_at(place, sign=1):
        return expert_at(place, sign) + ds[place[2]]

    half = w_in.shape[1]
    loads = [
        pltpu.make_async_copy(tokens_h.at[0], tok, load_sem.at[0]),
        pltpu.make_async_copy(router_h, router, load_sem.at[1]),
        pltpu.make_async_copy(b_in_h.at[:, pl.ds(pl.multiple_of(dp * half, half), half)], b_in, load_sem.at[2]),
        pltpu.make_async_copy(b_out_h, b_out, load_sem.at[3]),
    ]
    weights = [
        pltpu.make_async_copy(w_in_h.at[0], w_in, w_sem.at[0]),
        pltpu.make_async_copy(w_out_h.at[0], w_out, w_sem.at[1]),
    ]
    for copy in loads[:2]:
        copy.start()
    ret[...] = jnp.zeros_like(ret)

    barrier = pltpu.get_barrier_semaphore()
    for place in sorted(SLOTS[1:], key=hops, reverse=True):
        pl.semaphore_signal(barrier, inc=1, device_id=device_at(place), device_id_type=LOGICAL)
    pl.semaphore_signal(barrier, inc=1, device_id=partner, device_id_type=LOGICAL)
    for copy in loads[2:] + weights:
        copy.start()

    self_block, self_row = 2 * SELF // EXPERTS, 2 * SELF % EXPERTS
    for copy in loads[:2]:
        copy.wait()
    logits = dot(tok[...], router[...])
    up = jnp.exp(logits - jnp.max(logits, axis=0, keepdims=True))
    dispatch = (up / jnp.sum(up, axis=0, keepdims=True)).astype(BF16)
    across = jnp.exp(logits - jnp.max(logits, axis=1, keepdims=True))
    combine = (across / jnp.sum(across, axis=1, keepdims=True)).astype(BF16)
    rows = None
    for h in range(2):
        lhs = dot_nt(spread_t((2 * EXPERTS, EXPERTS), h), dispatch).astype(BF16)
        term = dot(lhs, tok[:, h * HALF : (h + 1) * HALF])
        rows = term if rows is None else rows + term
        comb2[h] = dot(combine, spread((EXPERTS, 2 * EXPERTS), h)).astype(BF16)
        pick = lax.broadcasted_iota(jnp.int32, (EXPERTS, EXPERTS), 0) == me
        into = lax.broadcasted_iota(jnp.int32, (EXPERTS, EXPERTS), 1) == self_row + h
        self2[h] = dot(combine, jnp.where(pick & into, 1.0, 0.0).astype(BF16)).astype(BF16)
    src[...] = rows.astype(BF16)
    mine = dot(one_hot((8, 2 * EXPERTS), lambda r: 2 * me + r), src[...]).astype(BF16)
    got[2 * SELF : 2 * SELF + 2, :] = mine[0:2, :]

    pl.semaphore_wait(barrier, len(SLOTS))

    for b, (first, count) in enumerate(BATCHES):
        for k in range(first, first + count):
            if k != SELF:
                pltpu.make_async_remote_copy(
                    src.at[pl.ds(pl.multiple_of(2 * expert_at(SLOTS[k]), 2), 2)],
                    got.at[pl.ds(2 * k, 2)],
                    send_sem, recv_sem.at[b],
                    device_id=device_at(SLOTS[k]), device_id_type=LOGICAL,
                ).start()

    width = w_in.shape[0]

    def forward(b):
        first, count = BATCHES[b]
        held = unit.at[pl.ds(0, count - 1 if first <= SELF < first + count else count)]
        pltpu.make_async_copy(held, held, recv_sem.at[b]).wait()
        block = pl.ds(2 * first, 2 * count)
        pltpu.make_async_remote_copy(
            got.at[block], got2.at[block], fsend_sem, frecv_sem.at[b], device_id=partner, device_id_type=LOGICAL
        ).start()

    def first_half(b):
        first, count = BATCHES[b]
        block = pl.ds(2 * first, 2 * count)
        pltpu.make_async_copy(got2.at[block], got2.at[block], frecv_sem.at[b]).wait()
        for h in range(2):
            order = spread((count, 2 * count), h)
            x[0:count, h * HALF : (h + 1) * HALF] = dot(order, got[block, :]).astype(BF16)
            x[count : 2 * count, h * HALF : (h + 1) * HALF] = dot(order, got2[block, :]).astype(BF16)
        if b == 0:
            loads[2].wait()
            weights[0].wait()
        step = 512
        for j in range(half // step):
            cols = slice(j * step, (j + 1) * step)
            acc = dot(x[0 : 2 * count], w_in[:, cols]) + b_in[:, cols].astype(F32)
            hidden[0 : 2 * count, cols] = gelu(acc).astype(BF16)

    def second_half(b):
        first, count = BATCHES[b]
        block = pl.ds(first, count)
        if b == 0:
            weights[1].wait()
        step = 256
        for j in range(width // step):
            cols = slice(j * step, (j + 1) * step)
            acc = dot(hidden[0 : 2 * count], w_out[:, cols])
            part[block, cols] = acc[0:count]
            psend[block, cols] = acc[count : 2 * count].astype(BF16)
        pltpu.make_async_remote_copy(
            psend.at[block], precv.at[block], psend_sem, precv_sem.at[b], device_id=partner, device_id_type=LOGICAL
        ).start()

    def send_back(b):
        first, count = BATCHES[b]
        block = pl.ds(first, count)
        pltpu.make_async_copy(precv.at[block], precv.at[block], precv_sem.at[b]).wait()
        if b == 0:
            loads[3].wait()
        result = (part[block, :] + precv[block, :].astype(F32) + b_out[...].astype(F32)).astype(BF16)
        rows = None
        for h in range(2):
            term = dot(spread_t((2 * count, count), h), result[:, h * HALF : (h + 1) * HALF])
            rows = term if rows is None else rows + term
        rsrc[pl.ds(2 * first, 2 * count), :] = rows.astype(BF16)
        for k in range(first, first + count):
            if k != SELF:
                pltpu.make_async_remote_copy(
                    rsrc.at[pl.ds(2 * k, 2)],
                    ret.at[pl.ds(pl.multiple_of(2 * me, 2), 2)],
                    rsend_sem, rrecv_sem,
                    device_id=device_at(SLOTS[k], -1), device_id_type=LOGICAL,
                ).start()

    stages = {"F": forward, "G": first_half, "H": second_half, "R": send_back}
    for stage in SCHEDULE:
        stages[stage[0]](int(stage[1:]))

    others = unit.at[pl.ds(0, EXPERTS - 1)]
    pltpu.make_async_copy(others, others, rrecv_sem).wait()
    for h in range(2):
        own = rsrc[self_block * EXPERTS : (self_block + 1) * EXPERTS, :]
        mixed = dot(comb2[h], ret[...]) + dot(self2[h], own)
        out_ref[:, h * HALF : (h + 1) * HALF] = mixed.astype(BF16)

    pltpu.make_async_copy(others, others, send_sem).wait()
    pltpu.make_async_copy(others, others, rsend_sem).wait()
    pltpu.make_async_copy(got, got, fsend_sem).wait()
    pltpu.make_async_copy(psend, psend, psend_sem).wait()


def layer(tokens, router, w_in, b_in, w_out, b_out):
    _, m, d = tokens.shape
    half = w_in.shape[2]
    anywhere = pl.BlockSpec(memory_space=pltpu.HBM)
    dma = pltpu.SemaphoreType.DMA
    out = pl.pallas_call(
        kernel,
        name="soft_moe",
        out_shape=jax.ShapeDtypeStruct((m, d), BF16),
        in_specs=[anywhere] * 6,
        out_specs=pl.BlockSpec(memory_space=pltpu.VMEM),
        scratch_shapes=[
            pltpu.VMEM((m, d), BF16),
            pltpu.VMEM((d, EXPERTS), BF16),
            pltpu.VMEM((d, half), BF16),
            pltpu.VMEM((half, d), BF16),
            pltpu.VMEM((1, half), BF16),
            pltpu.VMEM((1, d), BF16),
            pltpu.VMEM((2 * EXPERTS, HALF), BF16),
            pltpu.VMEM((2 * EXPERTS, HALF), BF16),
            pltpu.VMEM((2 * EXPERTS, HALF), BF16),
            pltpu.VMEM((2 * max(SIZES), d), BF16),
            pltpu.VMEM((2 * max(SIZES), half), BF16),
            pltpu.VMEM((EXPERTS, d), F32),
            pltpu.VMEM((EXPERTS, d), BF16),
            pltpu.VMEM((EXPERTS, d), BF16),
            pltpu.VMEM((2 * EXPERTS, HALF), BF16),
            pltpu.VMEM((2 * EXPERTS, HALF), BF16),
            pltpu.VMEM((2, m, 2 * EXPERTS), BF16),
            pltpu.VMEM((2, m, EXPERTS), BF16),
            pltpu.VMEM((EXPERTS, 2, HALF), BF16),
            dma((4,)), dma((2,)),
            dma, dma((len(SIZES),)),
            dma, dma((len(SIZES),)),
            dma, dma((len(SIZES),)),
            dma, dma,
        ],
        compiler_params=pltpu.CompilerParams(
            collective_id=1, has_side_effects=True, vmem_limit_bytes=67043328
        ),
    )(tokens, router, w_in, b_in, w_out, b_out)
    return out[None]


def solution(mesh):
    finer = Mesh(mesh.devices.reshape(mesh.shape["dp"], NY, NZ, 2, 2), AXES)
    return jax.shard_map(
        layer,
        mesh=finer,
        in_specs=(
            P(AXES, None, None),
            P(),
            P(EXPERT, None, "dp"),
            P(EXPERT, None),
            P(EXPERT, "dp", None),
            P(EXPERT, None),
        ),
        out_specs=P(AXES, None, None),
        check_vma=False,
    )
```
